32 devices in a mesh: dp: 1 (over z), cy: 4 (over y), cx: 8 (over x, core).
Axes of the slice: x: 4, y: 4, z: 1, core: 2. Of those that a mesh axis runs over, the one named last changes fastest.
The devices are a block of a 4x4x8 slice.
Arguments:
- q: bfloat16 [4096, 40, 128], P(('dp', 'cy', 'cx'))
- k: bfloat16 [4096, 40, 128], P(('dp', 'cy', 'cx'))
- v: bfloat16 [4096, 40, 128], P(('dp', 'cy', 'cx'))
Outputs:
- output: bfloat16 [4096, 40, 128], P(('dp', 'cy', 'cx'))
All inputs are finite; a program needn't handle non-finite values.
Results may differ from the reference program's by a relative error of at most 0.00345903.
Values are sent between devices in bfloat16 or wider.
A program may use at most 768 MiB of HBM per device.

```python
import jax
import jax.numpy as jnp
from jax import lax

SEQ = 4096
NDEV = 32
HEADS = 40
KV_HEADS = 40
HEAD_DIM = 128

SPAN = SEQ // (2 * NDEV)
NEG = -1.0e30


def positions():
    i = jnp.arange(SEQ)
    blk = i // (2 * SPAN)
    j = i % (2 * SPAN)
    return jnp.where(j < SPAN, blk * SPAN + j, (2 * NDEV - 1 - blk) * SPAN + j - SPAN)


def setup_inputs(seed: int = 0, part: int = 0) -> dict:
    key = jax.random.fold_in(jax.random.key(seed), part)
    kq, kk, kv, ko = jax.random.split(key, 4)
    q = jax.random.normal(kq, (SEQ, HEADS, HEAD_DIM), jnp.float32)
    k = jax.random.normal(kk, (SEQ, KV_HEADS, HEAD_DIM), jnp.float32)
    off = jax.random.normal(ko, (2 * NDEV, 1, KV_HEADS, HEAD_DIM), jnp.float32)
    v = 0.5 * jax.random.normal(kv, (2 * NDEV, SPAN, KV_HEADS, HEAD_DIM), jnp.float32) + off
    v = v.reshape(SEQ, KV_HEADS, HEAD_DIM)
    return {'q': q.astype(jnp.bfloat16), 'k': k.astype(jnp.bfloat16), 'v': v.astype(jnp.bfloat16)}


def reference(q, k, v):
    rep = HEADS // KV_HEADS
    scale = HEAD_DIM ** -0.5
    pos = positions().reshape(2 * NDEV, SPAN)
    qc = q.reshape(2 * NDEV, SPAN, KV_HEADS, rep, HEAD_DIM)
    kc = k.reshape(2 * NDEV, SPAN, KV_HEADS, HEAD_DIM)
    vc = v.reshape(2 * NDEV, SPAN, KV_HEADS, HEAD_DIM)

    def one_query_span(xs):
        qb, pq = xs
        qf = qb.astype(jnp.float32)

        def step(carry, ys):
            m, l, acc = carry
            kb, vb, pk = ys
            s = jnp.einsum('qgrd,kgd->grqk', qf, kb.astype(jnp.float32)) * scale
            mask = pk[None, :] <= pq[:, None]
            s = jnp.where(mask, s, NEG)
            mn = jnp.maximum(m, jnp.max(s, axis=-1))
            p = jnp.where(mask, jnp.exp(s - mn[..., None]), 0.0)
            alpha = jnp.exp(m - mn)
            l = alpha * l + jnp.sum(p, axis=-1)
            pv = jnp.einsum('grqk,kgd->grqd', p.astype(jnp.bfloat16).astype(jnp.float32), vb.astype(jnp.float32))
            acc = alpha[..., None] * acc + pv
            return (mn, l, acc), None

        init = (jnp.full((KV_HEADS, rep, SPAN), NEG, jnp.float32),
                jnp.zeros((KV_HEADS, rep, SPAN), jnp.float32),
                jnp.zeros((KV_HEADS, rep, SPAN, HEAD_DIM), jnp.float32))
        (m, l, acc), _ = lax.scan(step, init, (kc, vc, pos))
        o = (acc / l[..., None]).astype(jnp.bfloat16)
        return o.transpose(2, 0, 1, 3).reshape(SPAN, HEADS, HEAD_DIM)

    out = lax.map(one_query_span, (qc, pos))
    return out.reshape(SEQ, HEADS, HEAD_DIM)
```

```python
import functools
import math

import jax
import jax.numpy as jnp
from jax import lax
from jax.experimental import pallas as pl
from jax.experimental.pallas import tpu as pltpu
from jax.sharding import PartitionSpec as P

MESH = pl.DeviceIdType.MESH
NEG = -1.0e30
TILE = 8
F32 = jnp.float32
BF16 = jnp.bfloat16


def kernel(ny, nx, nt, scale, q_hbm, k_hbm, v_hbm, o_hbm, tin, xs, send, qkv, sbuf, bias, ostage, orecv, ys, tout,
           in_sem, send_sem, recv_sem, fsend, frecv, osend, orecv_sem, out_sem):
    rows = q_hbm.shape[0]
    c2 = rows // 2
    hd = q_hbm.shape[2]
    ns = ny * nx
    cy = lax.axis_index("cy")
    cx = lax.axis_index("cx")
    x = cx // 2
    c = lax.rem(cx, 2)
    par = lax.rem(x + cy, 2)
    me = cy * nx + x
    pair = cy * (nx // 2) + x // 2
    nslots = (nt - par + 1) // 2

    def dev(s, core):
        return {"cy": s // nx, "cx": lax.rem(s, nx) * 2 + core}

    def in_copy(t, j):
        src = (q_hbm, k_hbm, v_hbm)[j]
        return pltpu.make_async_copy(src.at[:, pl.ds(pl.multiple_of(t * TILE, TILE), TILE), :], tin.at[t, j], in_sem.at[t, j])

    for t in range(nt):
        for j in range(3):
            in_copy(t, j).start()

    bar = pltpu.get_barrier_semaphore()

    def greet(i, _):
        pl.semaphore_signal(bar, inc=1, device_id=dev(lax.rem(me + i, ns), c), device_id_type=MESH)
        return 0

    lax.fori_loop(1, ns, greet, 0)
    pl.semaphore_signal(bar, inc=1, device_id=dev(me, 1 - c), device_id_type=MESH)

    qi = lax.broadcasted_iota(jnp.int32, (nx * c2, 2 * nx * c2), 0)
    ki = lax.broadcasted_iota(jnp.int32, (nx * c2, 2 * nx * c2), 1)
    qsp = 2 * (qi // c2) + c
    ksp = 2 * ((ki // c2) % nx) + ki // (nx * c2)
    qr = qi % c2
    kr = ki % c2
    low = (ksp < qsp) | ((ksp == qsp) & (kr <= qr))
    high = (ksp > qsp) | ((ksp == qsp) & (kr <= qr))
    bias[0] = jnp.where(low, 0.0, NEG)
    bias[1] = jnp.where(high, 0.0, NEG)

    def send_copy(t, k):
        yd = k // (nx // 2)
        xd = 2 * lax.rem(k, nx // 2) + lax.rem(yd + t, 2)
        d = yd * nx + xd
        slot = t // 2
        return d, slot, pltpu.make_async_remote_copy(
            src_ref=send.at[t, k], dst_ref=qkv.at[slot, c, me], send_sem=send_sem.at[t, k],
            recv_sem=recv_sem.at[slot, me], device_id=dev(d, c), device_id_type=MESH)

    def send_tile(t, _):
        for j in range(3):
            in_copy(t, j).wait()
            xs[j] = tin[t, j].astype(F32).reshape(rows * TILE, hd)

        def one(i, _):
            yd = lax.rem(cy + i // (nx // 2), ny)
            k = yd * (nx // 2) + lax.rem(x // 2 + i, nx // 2)
            d, slot, cp = send_copy(t, k)
            for j in range(3):
                send[t, k, j] = xs[j, pl.ds(k, rows, stride=TILE), :].astype(BF16).reshape(2, c2, hd)

            @pl.when(d != me)
            def _():
                cp.start()

            @pl.when(d == me)
            def _():
                qkv[slot, c, me] = send[t, k]
            return 0

        lax.fori_loop(0, TILE, one, 0)
        return 0

    pl.semaphore_wait(bar, ns)
    lax.fori_loop(0, nt, send_tile, 0)

    def fwd_copy(slot, s, core):
        return pltpu.make_async_remote_copy(
            src_ref=qkv.at[slot, core, s, pl.ds(1, 2)], dst_ref=qkv.at[slot, core, s, pl.ds(1, 2)],
            send_sem=fsend.at[slot, s], recv_sem=frecv.at[slot, s], device_id=dev(me, 1 - c), device_id_type=MESH)

    def recv_copy(slot, s):
        return pltpu.make_async_remote_copy(
            src_ref=qkv.at[slot, c, s], dst_ref=qkv.at[slot, c, s], send_sem=send_sem.at[0, 0],
            recv_sem=recv_sem.at[slot, s], device_id=dev(me, 1 - c), device_id_type=MESH)

    def o_copy(slot, s):
        t = 2 * slot + par
        return pltpu.make_async_remote_copy(
            src_ref=ostage.at[slot, s], dst_ref=orecv.at[t, pair], send_sem=osend.at[slot, s],
            recv_sem=orecv_sem.at[t, pair], device_id=dev(s, c), device_id_type=MESH)

    def band(slot, b, j):
        half = b // ny
        yk = jnp.where(half == 0, b, 2 * ny - 1 - b)
        return qkv[slot, :, pl.ds(nx * yk, nx), j, half].reshape(2 * nx * c2, hd)

    def scores(q, k):
        return lax.dot_general(q, k, (((1,), (1,)), ((), ())), preferred_element_type=F32) * scale

    def lanes(s, op):
        r = s[:, :hd]
        for i in range(1, s.shape[1] // hd):
            r = op(r, s[:, i * hd:(i + 1) * hd])
        return r

    def attend(slot, y, half):
        j = y if half == 0 else 2 * ny - 1 - y
        q = qkv[slot, c, pl.ds(nx * y, nx), 0, half].reshape(nx * c2, hd)
        s = scores(q, band(slot, j, 1)) + bias[half]
        sbuf[j] = s
        mx = lanes(s, jnp.maximum)

        def first(b, mx):
            s = scores(q, band(slot, b, 1))
            sbuf[b] = s
            return jnp.maximum(mx, lanes(s, jnp.maximum))

        mx = lax.fori_loop(0, j, first, mx)
        m = jnp.max(mx, axis=-1, keepdims=True)

        def second(b, carry):
            l, acc = carry
            p = jnp.exp2(sbuf[b] - m)
            l = l + lanes(p, jnp.add)
            acc = acc + jnp.dot(p.astype(BF16), band(slot, b, 2), preferred_element_type=F32)
            return l, acc

        zero = jnp.zeros((nx * c2, hd), F32)
        l, acc = lax.fori_loop(0, j + 1, second, (zero, zero))
        o = acc / jnp.sum(l, axis=-1, keepdims=True)
        ostage[slot, pl.ds(nx * y, nx), half] = o.astype(BF16).reshape(nx, c2, hd)

    def do_slot(slot, _):
        def forward(s, _):
            @pl.when(s != me)
            def _():
                recv_copy(slot, s).wait_recv()

            fwd_copy(slot, s, c).start()
            return 0

        lax.fori_loop(0, ns, forward, 0)

        def arrived(s, _):
            fwd_copy(slot, s, 1 - c).wait_recv()
            return 0

        lax.fori_loop(0, ns, arrived, 0)

        def rows_of(y, _):
            attend(slot, y, 0)
            attend(slot, y, 1)

            def back(i, _):
                s = nx * y + i

                @pl.when(s != me)
                def _():
                    o_copy(slot, s).start()

                @pl.when(s == me)
                def _():
                    orecv[2 * slot + par, pair] = ostage[slot, s]
                return 0

            lax.fori_loop(0, nx, back, 0)
            return 0

        lax.fori_loop(0, ny, rows_of, 0)
        return 0

    lax.fori_loop(0, nslots, do_slot, 0)

    def out_copy(t):
        return pltpu.make_async_copy(tout.at[t], o_hbm.at[:, pl.ds(pl.multiple_of(t * TILE, TILE), TILE), :], out_sem.at[t])

    def out_tile(t, _):
        def one(k, _):
            yd = k // (nx // 2)
            d = yd * nx + 2 * lax.rem(k, nx // 2) + lax.rem(yd + t, 2)

            @pl.when(d != me)
            def _():
                pltpu.make_async_remote_copy(
                    src_ref=orecv.at[t, k], dst_ref=orecv.at[t, k], send_sem=osend.at[0, 0],
                    recv_sem=orecv_sem.at[t, k], device_id=dev(me, 1 - c), device_id_type=MESH).wait_recv()

            ys[pl.ds(k, rows, stride=TILE), :] = orecv[t, k].reshape(rows, hd).astype(F32)
            return 0

        lax.fori_loop(0, TILE, one, 0)
        tout[t] = ys[...].reshape(rows, TILE, hd).astype(BF16)
        out_copy(t).start()
        return 0

    lax.fori_loop(0, nt, out_tile, 0)

    def sent(t, _):
        def one(k, _):
            d, slot, cp = send_copy(t, k)

            @pl.when(d != me)
            def _():
                cp.wait_send()
            return 0

        lax.fori_loop(0, TILE, one, 0)
        out_copy(t).wait()
        return 0

    lax.fori_loop(0, nt, sent, 0)

    def drained(slot, _):
        def one(s, _):
            fwd_copy(slot, s, c).wait_send()

            @pl.when(s != me)
            def _():
                o_copy(slot, s).wait_send()
            return 0

        lax.fori_loop(0, ns, one, 0)
        return 0

    lax.fori_loop(0, nslots, drained, 0)


def solution(mesh):
    ny = mesh.shape['cy']
    nx = mesh.shape['cx'] // 2
    spec = P(('dp', 'cy', 'cx'))

    def local(q, k, v):
        rows, nh, hd = q.shape
        c2 = rows // 2
        nt = nh // TILE
        ns = ny * nx
        nslot = (nt + 1) // 2
        scale = hd ** -0.5 * math.log2(math.e)
        dma = pltpu.SemaphoreType.DMA
        return pl.pallas_call(
            functools.partial(kernel, ny, nx, nt, scale),
            out_shape=jax.ShapeDtypeStruct(q.shape, q.dtype),
            in_specs=[pl.BlockSpec(memory_space=pl.ANY)] * 3,
            out_specs=pl.BlockSpec(memory_space=pl.ANY),
            scratch_shapes=[
                pltpu.VMEM((nt, 3, rows, TILE, hd), BF16),
                pltpu.VMEM((3, rows * TILE, hd), F32),
                pltpu.VMEM((nt, TILE, 3, 2, c2, hd), BF16),
                pltpu.VMEM((nslot, 2, ns, 3, 2, c2, hd), BF16),
                pltpu.VMEM((2 * ny, nx * c2, 2 * nx * c2), F32),
                pltpu.VMEM((2, nx * c2, 2 * nx * c2), F32),
                pltpu.VMEM((nslot, ns, 2, c2, hd), BF16),
                pltpu.VMEM((nt, TILE, 2, c2, hd), BF16),
                pltpu.VMEM((rows * TILE, hd), F32),
                pltpu.VMEM((nt, rows, TILE, hd), BF16),
                dma((nt, 3)), dma((nt, TILE)), dma((nslot, ns)), dma((nslot, ns)), dma((nslot, ns)),
                dma((nslot, ns)), dma((nt, TILE)), dma((nt,)),
            ],
            compiler_params=pltpu.CompilerParams(collective_id=0, has_side_effects=True, vmem_limit_bytes=56 * 1024 * 1024),
        )(q, k, v)

    return jax.shard_map(local, mesh=mesh, in_specs=(spec, spec, spec), out_specs=spec, check_vma=False)
```

```python
import functools
import math

import jax
import jax.numpy as jnp
from jax import lax
from jax.experimental import pallas as pl
from jax.experimental.pallas import tpu as pltpu
from jax.sharding import PartitionSpec as P

MESH = pl.DeviceIdType.MESH
NEG = -1.0e30
TILE = 8
F32 = jnp.float32
BF16 = jnp.bfloat16


def kernel(ny, nx, nt, scale, q_hbm, k_hbm, v_hbm, o_hbm, tin, xs, send, qkv, sbuf, bias, mbuf, lbuf, abuf, ostage, orecv, ys, tout,
           in_sem, send_sem, recv_sem, fsend, frecv, osend, orecv_sem, out_sem):
    rows = q_hbm.shape[0]
    c2 = rows // 2
    hd = q_hbm.shape[2]
    ns = ny * nx
    cy = lax.axis_index("cy")
    cx = lax.axis_index("cx")
    x = cx // 2
    c = lax.rem(cx, 2)
    par = lax.rem(x + cy, 2)
    me = cy * nx + x
    pair = cy * (nx // 2) + x // 2
    nslots = (nt - par + 1) // 2

    def dev(s, core):
        return {"cy": s // nx, "cx": lax.rem(s, nx) * 2 + core}

    def in_copy(t, j):
        src = (q_hbm, k_hbm, v_hbm)[j]
        return pltpu.make_async_copy(src.at[:, pl.ds(pl.multiple_of(t * TILE, TILE), TILE), :], tin.at[t, j], in_sem.at[t, j])

    for t in range(nt):
        for j in range(3):
            in_copy(t, j).start()

    bar = pltpu.get_barrier_semaphore()

    def greet(i, _):
        pl.semaphore_signal(bar, inc=1, device_id=dev(lax.rem(me + i, ns), c), device_id_type=MESH)
        return 0

    lax.fori_loop(1, ns, greet, 0)
    pl.semaphore_signal(bar, inc=1, device_id=dev(me, 1 - c), device_id_type=MESH)

    qi = lax.broadcasted_iota(jnp.int32, (nx * c2, 2 * nx * c2), 0)
    ki = lax.broadcasted_iota(jnp.int32, (nx * c2, 2 * nx * c2), 1)
    qsp = 2 * (qi // c2) + c
    ksp = 2 * ((ki // c2) % nx) + ki // (nx * c2)
    qr = qi % c2
    kr = ki % c2
    low = (ksp < qsp) | ((ksp == qsp) & (kr <= qr))
    high = (ksp > qsp) | ((ksp == qsp) & (kr <= qr))
    bias[0] = jnp.where(low, 0.0, NEG)
    bias[1] = jnp.where(high, 0.0, NEG)

    def send_copy(t, k):
        yd = k // (nx // 2)
        xd = 2 * lax.rem(k, nx // 2) + lax.rem(yd + t, 2)
        d = yd * nx + xd
        slot = t // 2
        return d, slot, pltpu.make_async_remote_copy(
            src_ref=send.at[t, k], dst_ref=qkv.at[slot, c, me], send_sem=send_sem.at[t, k],
            recv_sem=recv_sem.at[slot, me], device_id=dev(d, c), device_id_type=MESH)

    def send_tile(t, _):
        for j in range(3):
            in_copy(t, j).wait()
            xs[j] = tin[t, j].astype(F32).reshape(rows * TILE, hd)

        def one(i, _):
            yd = lax.rem(cy + i // (nx // 2), ny)
            k = yd * (nx // 2) + lax.rem(x // 2 + i, nx // 2)
            d, slot, cp = send_copy(t, k)
            for j in range(3):
                send[t, k, j] = xs[j, pl.ds(k, rows, stride=TILE), :].astype(BF16).reshape(2, c2, hd)

            @pl.when(d != me)
            def _():
                cp.start()

            @pl.when(d == me)
            def _():
                qkv[slot, c, me] = send[t, k]
            return 0

        lax.fori_loop(0, TILE, one, 0)
        return 0

    pl.semaphore_wait(bar, ns)
    lax.fori_loop(0, nt, send_tile, 0)

    def fwd_copy(slot, s, core):
        return pltpu.make_async_remote_copy(
            src_ref=qkv.at[slot, core, s, pl.ds(1, 2)], dst_ref=qkv.at[slot, core, s, pl.ds(1, 2)],
            send_sem=fsend.at[slot, s], recv_sem=frecv.at[slot, s], device_id=dev(me, 1 - c), device_id_type=MESH)

    def recv_copy(slot, s):
        return pltpu.make_async_remote_copy(
            src_ref=qkv.at[slot, c, s], dst_ref=qkv.at[slot, c, s], send_sem=send_sem.at[0, 0],
            recv_sem=recv_sem.at[slot, s], device_id=dev(me, 1 - c), device_id_type=MESH)

    def o_copy(slot, s):
        t = 2 * slot + par
        return pltpu.make_async_remote_copy(
            src_ref=ostage.at[slot, s], dst_ref=orecv.at[t, pair], send_sem=osend.at[slot, s],
            recv_sem=orecv_sem.at[t, pair], device_id=dev(s, c), device_id_type=MESH)

    def band(slot, b, j):
        half = b // ny
        yk = jnp.where(half == 0, b, 2 * ny - 1 - b)
        return qkv[slot, :, pl.ds(nx * yk, nx), j, half].reshape(2 * nx * c2, hd)

    def scores(q, k):
        return lax.dot_general(q, k, (((1,), (1,)), ((), ())), preferred_element_type=F32) * scale

    def lanes(s, op):
        r = s[:, :hd]
        for i in range(1, s.shape[1] // hd):
            r = op(r, s[:, i * hd:(i + 1) * hd])
        return r

    def attend(slot, y):
        last = 2 * ny - 1
        blocks = [(0, y, 0), (1, last - y, 1)]
        for n in range(last):
            high = (n >= y).astype(jnp.int32)
            blocks.append((high, n - high * y, None))
        for n, (half, b, mask) in enumerate(blocks):
            q = qkv[slot, c, pl.ds(nx * y, nx), 0, half].reshape(nx * c2, hd)
            s = scores(q, band(slot, b, 1))
            if mask is not None:
                s = s + bias[mask]
            sbuf[n] = s
            mx = lanes(s, jnp.maximum)
            mbuf[half] = mx if mask is not None else jnp.maximum(mbuf[half], mx)
        for half in range(2):
            mbuf[half] = jnp.broadcast_to(jnp.max(mbuf[half], axis=-1, keepdims=True), (nx * c2, hd))
        for n, (half, b, mask) in enumerate(blocks):
            m = mbuf[half]
            p = jnp.exp2(sbuf[n] - jnp.concatenate([m] * (sbuf.shape[2] // hd), axis=1))
            l = lanes(p, jnp.add)
            pv = jnp.dot(p.astype(BF16), band(slot, b, 2), preferred_element_type=F32)
            if mask is None:
                l = lbuf[half] + l
                pv = abuf[half] + pv
            lbuf[half] = l
            abuf[half] = pv
        for half in range(2):
            o = abuf[half] / jnp.sum(lbuf[half], axis=-1, keepdims=True)
            ostage[slot, pl.ds(nx * y, nx), half] = o.astype(BF16).reshape(nx, c2, hd)

    def do_slot(slot, _):
        def forward(s, _):
            @pl.when(s != me)
            def _():
                recv_copy(slot, s).wait_recv()

            fwd_copy(slot, s, c).start()
            return 0

        lax.fori_loop(0, ns, forward, 0)

        def arrived(s, _):
            fwd_copy(slot, s, 1 - c).wait_recv()
            return 0

        lax.fori_loop(0, ns, arrived, 0)

        def rows_of(y, _):
            attend(slot, y)

            def back(i, _):
                s = nx * y + i

                @pl.when(s != me)
                def _():
                    o_copy(slot, s).start()

                @pl.when(s == me)
                def _():
                    orecv[2 * slot + par, pair] = ostage[slot, s]
                return 0

            lax.fori_loop(0, nx, back, 0)
            return 0

        lax.fori_loop(0, ny, rows_of, 0)
        return 0

    lax.fori_loop(0, nslots, do_slot, 0)

    def out_copy(t):
        return pltpu.make_async_copy(tout.at[t], o_hbm.at[:, pl.ds(pl.multiple_of(t * TILE, TILE), TILE), :], out_sem.at[t])

    def out_tile(t, _):
        def one(k, _):
            yd = k // (nx // 2)
            d = yd * nx + 2 * lax.rem(k, nx // 2) + lax.rem(yd + t, 2)

            @pl.when(d != me)
            def _():
                pltpu.make_async_remote_copy(
                    src_ref=orecv.at[t, k], dst_ref=orecv.at[t, k], send_sem=osend.at[0, 0],
                    recv_sem=orecv_sem.at[t, k], device_id=dev(me, 1 - c), device_id_type=MESH).wait_recv()

            ys[pl.ds(k, rows, stride=TILE), :] = orecv[t, k].reshape(rows, hd).astype(F32)
            return 0

        lax.fori_loop(0, TILE, one, 0)
        tout[t] = ys[...].reshape(rows, TILE, hd).astype(BF16)
        out_copy(t).start()
        return 0

    lax.fori_loop(0, nt, out_tile, 0)

    def sent(t, _):
        def one(k, _):
            d, slot, cp = send_copy(t, k)

            @pl.when(d != me)
            def _():
                cp.wait_send()
            return 0

        lax.fori_loop(0, TILE, one, 0)
        out_copy(t).wait()
        return 0

    lax.fori_loop(0, nt, sent, 0)

    def drained(slot, _):
        def one(s, _):
            fwd_copy(slot, s, c).wait_send()

            @pl.when(s != me)
            def _():
                o_copy(slot, s).wait_send()
            return 0

        lax.fori_loop(0, ns, one, 0)
        return 0

    lax.fori_loop(0, nslots, drained, 0)


def solution(mesh):
    ny = mesh.shape['cy']
    nx = mesh.shape['cx'] // 2
    spec = P(('dp', 'cy', 'cx'))

    def local(q, k, v):
        rows, nh, hd = q.shape
        c2 = rows // 2
        nt = nh // TILE
        ns = ny * nx
        nslot = (nt + 1) // 2
        scale = hd ** -0.5 * math.log2(math.e)
        dma = pltpu.SemaphoreType.DMA
        return pl.pallas_call(
            functools.partial(kernel, ny, nx, nt, scale),
            out_shape=jax.ShapeDtypeStruct(q.shape, q.dtype),
            in_specs=[pl.BlockSpec(memory_space=pl.ANY)] * 3,
            out_specs=pl.BlockSpec(memory_space=pl.ANY),
            scratch_shapes=[
                pltpu.VMEM((nt, 3, rows, TILE, hd), BF16),
                pltpu.VMEM((3, rows * TILE, hd), F32),
                pltpu.VMEM((nt, TILE, 3, 2, c2, hd), BF16),
                pltpu.VMEM((nslot, 2, ns, 3, 2, c2, hd), BF16),
                pltpu.VMEM((2 * ny + 1, nx * c2, 2 * nx * c2), F32),
                pltpu.VMEM((2, nx * c2, 2 * nx * c2), F32),
                pltpu.VMEM((2, nx * c2, hd), F32),
                pltpu.VMEM((2, nx * c2, hd), F32),
                pltpu.VMEM((2, nx * c2, hd), F32),
                pltpu.VMEM((nslot, ns, 2, c2, hd), BF16),
                pltpu.VMEM((nt, TILE, 2, c2, hd), BF16),
                pltpu.VMEM((rows * TILE, hd), F32),
                pltpu.VMEM((nt, rows, TILE, hd), BF16),
                dma((nt, 3)), dma((nt, TILE)), dma((nslot, ns)), dma((nslot, ns)), dma((nslot, ns)),
                dma((nslot, ns)), dma((nt, TILE)), dma((nt,)),
            ],
            compiler_params=pltpu.CompilerParams(collective_id=0, has_side_effects=True, vmem_limit_bytes=56 * 1024 * 1024),
        )(q, k, v)

    return jax.shard_map(local, mesh=mesh, in_specs=(spec, spec, spec), out_specs=spec, check_vma=False)
```

```python
import functools
import math

import jax
import jax.numpy as jnp
from jax import lax
from jax.experimental import pallas as pl
from jax.experimental.pallas import tpu as pltpu
from jax.sharding import PartitionSpec as P

MESH = pl.DeviceIdType.MESH
NEG = -1.0e30
TILE = 8
F32 = jnp.float32
BF16 = jnp.bfloat16


def kernel(ny, nx, nt, scale, q_hbm, k_hbm, v_hbm, o_hbm, tin, xs, send, r1, qkv, sbuf, bias, ostage, orecv, ys, tout,
           in_sem, s1, q1, s2, q2, sx, fsend, frecv, osend, orecv_sem, out_sem):
    rows = q_hbm.shape[0]
    c2 = rows // 2
    hd = q_hbm.shape[2]
    cy = lax.axis_index("cy")
    cx = lax.axis_index("cx")
    x = cx // 2
    c = lax.rem(cx, 2)
    odd = lax.rem(x + cy, 2)
    mate = cy + 1 - 2 * lax.rem(cy, 2)
    across = ny - 1 - cy
    inner = lax.rem((cy + 1) // 2, 2)

    def dev(xd, yd, core):
        return {"cy": yd, "cx": xd * 2 + core}

    nslot = (nt - 1) // 2

    def slot_of(t):
        return jnp.where(t == 0, nslot, (t - 1) // 2)

    def owner_row(t, xd, h, y, inn):
        shared = jnp.where(inn == h, y, y + 1 - 2 * lax.rem(y, 2))
        return jnp.where(t == 0, shared, lax.rem(xd + t, 2) + 2 * h)

    def in_copy(t, j):
        src = (q_hbm, k_hbm, v_hbm)[j]
        return pltpu.make_async_copy(src.at[:, pl.ds(pl.multiple_of(t * TILE, TILE), TILE), :], tin.at[t, j], in_sem.at[t, j])

    bar = pltpu.get_barrier_semaphore()
    for i in range(1, nx):
        pl.semaphore_signal(bar, inc=1, device_id=dev(lax.rem(x + i, nx), cy, c), device_id_type=MESH)
    for i in range(1, ny):
        pl.semaphore_signal(bar, inc=1, device_id=dev(x, lax.rem(cy + i, ny), c), device_id_type=MESH)
    pl.semaphore_signal(bar, inc=1, device_id=dev(x, cy, 1 - c), device_id_type=MESH)

    for t in range(nt):
        for j in range(3):
            in_copy(t, j).start()

    def x_copy(t, xd):
        return pltpu.make_async_remote_copy(
            src_ref=send.at[t, xd], dst_ref=r1.at[t, x], send_sem=s1.at[t, xd], recv_sem=q1.at[t, x],
            device_id=dev(xd, cy, c), device_id_type=MESH)

    def gray(i):
        return jnp.where(i < 2, i, 5 - i)

    def load_tile(t, u):
        for j in range(3):
            in_copy(t, j).wait()
            xs[u, j] = tin[t, j].astype(F32).reshape(rows * TILE, hd)

    def head_rows(u, j, k):
        return xs[u, j, pl.ds(k, rows, stride=TILE), :].astype(BF16).reshape(2, c2, hd)

    def send_tiles(t, n):
        def one(i, _):
            xd = lax.rem(x + gray(i), nx)
            for u in range(n):
                for h in range(2):
                    for j in range(3):
                        send[t + u, xd, h, j] = head_rows(u, j, 2 * xd + h)
                x_copy(t + u, xd).start()
            return 0

        lax.fori_loop(1, nx, one, 0)
        for u in range(n):
            for h in range(2):
                for j in range(3):
                    r1[t + u, x, h, j] = head_rows(u, j, 2 * x + h)

    load_tile(0, 0)

    qi = lax.broadcasted_iota(jnp.int32, (nx * c2, 2 * nx * c2), 0)
    ki = lax.broadcasted_iota(jnp.int32, (nx * c2, 2 * nx * c2), 1)
    qsp = 2 * (qi // c2) + c
    ksp = 2 * ((ki // c2) % nx) + ki // (nx * c2)
    qr = qi % c2
    kr = ki % c2
    low = (ksp < qsp) | ((ksp == qsp) & (kr <= qr))
    high = (ksp > qsp) | ((ksp == qsp) & (kr <= qr))
    bias[0] = jnp.where(low, 0.0, NEG)
    bias[1] = jnp.where(high, 0.0, NEG)

    pl.semaphore_wait(bar, nx + ny - 1)
    send_tiles(0, 1)

    def send_rest(i, _):
        load_tile(2 * i + 1, 0)
        load_tile(2 * i + 2, 1)
        send_tiles(2 * i + 1, 2)
        return 0

    lax.fori_loop(0, nslot, send_rest, 0)

    def y_copy(t, sx_, h, yd):
        slot = slot_of(t)
        return pltpu.make_async_remote_copy(
            src_ref=r1.at[t, sx_, h], dst_ref=qkv.at[slot, c, cy, sx_], send_sem=s2.at[t, sx_, h],
            recv_sem=q2.at[slot, cy, sx_], device_id=dev(x, yd, c), device_id_type=MESH)

    def y_recv(slot, sy, sx_):
        return pltpu.make_async_remote_copy(
            src_ref=qkv.at[slot, c, sy, sx_], dst_ref=qkv.at[slot, c, sy, sx_], send_sem=s2.at[0, 0, 0],
            recv_sem=q2.at[slot, sy, sx_], device_id=dev(x, cy, 1 - c), device_id_type=MESH)

    def kv_view(ref, full):
        return ref.at[pl.ds(1, 2)] if full else ref.at[pl.ds(1, 2), 0]

    def cross_copy(src, sy, sx_, full):
        return pltpu.make_async_remote_copy(
            src_ref=kv_view(src, full), dst_ref=kv_view(qkv.at[nslot, c, sy, sx_], full), send_sem=sx.at[sy, sx_],
            recv_sem=q2.at[nslot, sy, sx_], device_id=dev(x, across, c), device_id_type=MESH)

    def core_copy(src, slot, sy, sx_, core, full):
        return pltpu.make_async_remote_copy(
            src_ref=kv_view(src, full), dst_ref=kv_view(qkv.at[slot, core, sy, sx_], full), send_sem=fsend.at[slot, sy, sx_],
            recv_sem=frecv.at[slot, sy, sx_], device_id=dev(x, cy, 1 - c), device_id_type=MESH)

    def either(full, act):
        @pl.when(full)
        def _():
            act(True)

        @pl.when(jnp.logical_not(full))
        def _():
            act(False)

    outer = cy < ny // 2

    def cross(src, sy, sx_):
        either(jnp.logical_not(outer), lambda full: cross_copy(src, sy, sx_, full).start())

    def relay(t, i):
        sx_ = lax.rem(x + gray(i), nx)

        @pl.when(sx_ != x)
        def _():
            pltpu.make_async_remote_copy(
                src_ref=send.at[t, 0], dst_ref=r1.at[t, sx_], send_sem=s1.at[0, 0], recv_sem=q1.at[t, sx_],
                device_id=dev(x, cy, 1 - c), device_id_type=MESH).wait_recv()

        slot = slot_of(t)
        for h in range(2):
            yd = owner_row(t, x, h, cy, inner)

            @pl.when(yd != cy)
            def _():
                y_copy(t, sx_, h, yd).start()

            @pl.when(yd == cy)
            def _():
                core_copy(r1.at[t, sx_, h], slot, cy, sx_, c, True).start()

                @pl.when(t == 0)
                def _():
                    cross(r1.at[t, sx_, h], cy, sx_)

                qkv[slot, c, cy, sx_] = r1[t, sx_, h]

    def share_first(i):
        sx_ = lax.rem(x + gray(i), nx)
        y_recv(nslot, mate, sx_).wait_recv()
        core_copy(qkv.at[nslot, c, mate, sx_], nslot, mate, sx_, c, True).start()
        cross(qkv.at[nslot, c, mate, sx_], mate, sx_)

    def share_second(i):
        sx_ = lax.rem(x + gray(i), nx)
        for sy in (across, across + 1 - 2 * lax.rem(across, 2)):
            def act(full):
                cross_copy(qkv.at[nslot, c, sy, sx_], sy, sx_, full).wait_recv()
                core_copy(qkv.at[nslot, c, sy, sx_], nslot, sy, sx_, c, full).start()

            either(outer, act)
        return 0

    def full_rows(slot, sy):
        return (slot < nslot) | outer | (sy >= ny // 2)

    def arrived(slot):
        def one(i, _):
            sy = i // nx
            sx_ = lax.rem(i, nx)
            either(full_rows(slot, sy), lambda full: core_copy(qkv.at[slot, 1 - c, sy, sx_], slot, sy, sx_, 1 - c, full).wait_recv())
            return 0

        lax.fori_loop(0, nx * ny, one, 0)

    def gather(slot):
        def one(i, _):
            sy = lax.rem(cy + i // nx, ny)
            sx_ = lax.rem(x + gray(lax.rem(i, nx)), nx)
            y_recv(slot, sy, sx_).wait_recv()
            core_copy(qkv.at[slot, c, sy, sx_], slot, sy, sx_, c, True).start()
            return 0

        lax.fori_loop(nx, nx * ny, one, 0)

    def tile_of(slot):
        return jnp.where(slot == nslot, 0, 2 * slot + 2 - odd)

    def my_head(slot):
        return 2 * x + jnp.where(slot == nslot, inner, cy // 2)

    def o_copy(slot, sy, sx_):
        t = tile_of(slot)
        k = my_head(slot)
        return pltpu.make_async_remote_copy(
            src_ref=ostage.at[slot, sy, sx_], dst_ref=orecv.at[t, k], send_sem=osend.at[slot, sy, sx_],
            recv_sem=orecv_sem.at[t, k], device_id=dev(sx_, sy, c), device_id_type=MESH)

    def band(slot, b, j):
        half = b // ny
        yk = b if half == 0 else 2 * ny - 1 - b
        return qkv[slot, :, yk, :, j, half].reshape(2 * nx * c2, hd)

    def scores(q, k):
        return lax.dot_general(q, k, (((1,), (1,)), ((), ())), preferred_element_type=F32) * scale

    def lanes(s, op):
        r = s[:, :hd]
        for i in range(1, s.shape[1] // hd):
            r = op(r, s[:, i * hd:(i + 1) * hd])
        return r

    def attend(slot, pair):
        for p in range(ny // 2):
            @pl.when(pair == p)
            def _():
                attend_rows(slot, (2 * p, 2 * p + 1))

    def attend_rows(slot, source_rows):
        tiles = [(y, half, 2 * ny - y if half else y + 1) for half in (1, 0) for y in source_rows]
        tiles.sort(key=lambda t: -t[2])
        start = [sum(t[2] for t in tiles[:i]) for i in range(len(tiles) + 1)]
        top = [None] * len(tiles)
        total = [None] * len(tiles)

        def score(i, b):
            y, half, nb = tiles[i]
            q = qkv[slot, c, y, :, 0, half].reshape(nx * c2, hd)
            s = scores(q, band(slot, b, 1))
            if b == nb - 1:
                s = s + bias[half]
            sbuf[start[i] + b] = s
            t = lanes(s, jnp.maximum)
            top[i] = t if top[i] is None else jnp.maximum(top[i], t)

        def weigh(i, b, m):
            p = jnp.exp2(sbuf[start[i] + b] - m)
            l = lanes(p, jnp.add)
            pv = jnp.dot(p.astype(BF16), band(slot, b, 2), preferred_element_type=F32)
            total[i] = (l, pv) if total[i] is None else (total[i][0] + l, total[i][1] + pv)

        for b in range(tiles[0][2]):
            score(0, b)
        for i, (y, half, nb) in enumerate(tiles):
            m = jnp.broadcast_to(jnp.max(top[i], axis=-1, keepdims=True), (nx * c2, hd))
            m = jnp.concatenate([m] * (sbuf.shape[2] // hd), axis=1)
            nxt = tiles[i + 1][2] if i + 1 < len(tiles) else 0
            for b in range(max(nb, nxt)):
                if b < nxt:
                    score(i + 1, b)
                if b < nb:
                    weigh(i, b, m)
            l, acc = total[i]
            o = acc / jnp.sum(l, axis=-1, keepdims=True)
            ostage[slot, y, :, half] = o.astype(BF16).reshape(nx, c2, hd)

    def send_back(slot, y):
        def back(sx_, _):
            mine = (sx_ == x) & (y == cy)

            @pl.when(jnp.logical_not(mine))
            def _():
                o_copy(slot, y, sx_).start()

            @pl.when(mine)
            def _():
                orecv[tile_of(slot), my_head(slot)] = ostage[slot, y, sx_]
            return 0

        lax.fori_loop(0, nx, back, 0)
        return 0

    def relay_two(n, i):
        relay(2 * n + 1, i)
        relay(2 * n + 2, i)

    relay(0, 0)
    relay_two(0, 0)

    def first(i, _):
        @pl.when(i < nx)
        def _():
            relay(0, i)

        @pl.when(i == nx - 1)
        def _():
            relay_two(1, 0)

        share_first(i - 1)
        return 0

    lax.fori_loop(1, nx + 1, first, 0)
    lax.fori_loop(1, nx, lambda i, _: (relay_two(0, i), 0)[1], 0)
    lax.fori_loop(0, nx, lambda i, _: share_second(i), 0)

    def step(n, _):
        pairs = ny // 2
        slot = jnp.where(n == 0, nslot, (n - 1) // pairs)
        pair = jnp.where(n == 0, cy // 2, lax.rem(n + 1, pairs))

        @pl.when(n == 0)
        def _():
            relay_two(1, 1)
            relay_two(1, 2)

        @pl.when(n == 1)
        def _():
            relay_two(1, 3)

        @pl.when((n == 1) | (n == 1 + pairs))
        def _():
            gather(slot)

        @pl.when(n != 2)
        def _():
            @pl.when(n != 2 + pairs)
            def _():
                arrived(slot)

        attend(slot, pair)
        send_back(slot, 2 * pair)
        send_back(slot, 2 * pair + 1)
        return 0

    lax.fori_loop(0, 1 + nslot * ny // 2, step, 0)

    def out_copy(t):
        return pltpu.make_async_copy(tout.at[t], o_hbm.at[:, pl.ds(pl.multiple_of(t * TILE, TILE), TILE), :], out_sem.at[t])

    def out_tile(t, _):
        def one(k, _):
            xd = k // 2
            yd = owner_row(t, xd, lax.rem(k, 2), cy, inner)

            @pl.when((xd != x) | (yd != cy))
            def _():
                pltpu.make_async_remote_copy(
                    src_ref=orecv.at[t, k], dst_ref=orecv.at[t, k], send_sem=osend.at[0, 0, 0],
                    recv_sem=orecv_sem.at[t, k], device_id=dev(x, cy, 1 - c), device_id_type=MESH).wait_recv()

            ys[pl.ds(k, rows, stride=TILE), :] = orecv[t, k].reshape(rows, hd).astype(F32)
            return 0

        lax.fori_loop(0, TILE, one, 0)
        tout[t] = ys[...].reshape(rows, TILE, hd).astype(BF16)
        out_copy(t).start()
        return 0

    lax.fori_loop(0, nt, out_tile, 0)

    def sent(t, _):
        def one(i, _):
            xd = lax.rem(x + i, nx)

            @pl.when(i > 0)
            def _():
                x_copy(t, xd).wait_send()

            for h in range(2):
                yd = owner_row(t, x, h, cy, inner)

                @pl.when(yd != cy)
                def _():
                    y_copy(t, xd, h, yd).wait_send()
            return 0

        lax.fori_loop(0, nx, one, 0)
        out_copy(t).wait()
        return 0

    lax.fori_loop(0, nt, sent, 0)

    def drained(slot, _):
        def one(i, _):
            sy = i // nx
            sx_ = lax.rem(i, nx)
            mine = (sy // 2) == (cy // 2)
            either(full_rows(slot, sy), lambda full: core_copy(qkv.at[slot, c, sy, sx_], slot, sy, sx_, c, full).wait_send())

            @pl.when((slot == nslot) & mine)
            def _():
                either(jnp.logical_not(outer), lambda full: cross_copy(qkv.at[nslot, c, sy, sx_], sy, sx_, full).wait_send())

            @pl.when(((slot < nslot) | mine) & ((sy != cy) | (sx_ != x)))
            def _():
                o_copy(slot, sy, sx_).wait_send()
            return 0

        lax.fori_loop(0, nx * ny, one, 0)
        return 0

    lax.fori_loop(0, nslot + 1, drained, 0)


def solution(mesh):
    ny = mesh.shape['cy']
    nx = mesh.shape['cx'] // 2
    spec = P(('dp', 'cy', 'cx'))

    def local(q, k, v):
        rows, nh, hd = q.shape
        c2 = rows // 2
        nt = nh // TILE
        nslot = (nt + 1) // 2
        scale = hd ** -0.5 * math.log2(math.e)
        dma = pltpu.SemaphoreType.DMA
        return pl.pallas_call(
            functools.partial(kernel, ny, nx, nt, scale),
            out_shape=jax.ShapeDtypeStruct(q.shape, q.dtype),
            in_specs=[pl.BlockSpec(memory_space=pl.ANY)] * 3,
            out_specs=pl.BlockSpec(memory_space=pl.ANY),
            scratch_shapes=[
                pltpu.VMEM((nt, 3, rows, TILE, hd), BF16),
                pltpu.VMEM((2, 3, rows * TILE, hd), F32),
                pltpu.VMEM((nt, nx, 2, 3, 2, c2, hd), BF16),
                pltpu.VMEM((nt, nx, 2, 3, 2, c2, hd), BF16),
                pltpu.VMEM((nslot, 2, ny, nx, 3, 2, c2, hd), BF16),
                pltpu.VMEM((4 * ny + 2, nx * c2, 2 * nx * c2), F32),
                pltpu.VMEM((2, nx * c2, 2 * nx * c2), F32),
                pltpu.VMEM((nslot, ny, nx, 2, c2, hd), BF16),
                pltpu.VMEM((nt, TILE, 2, c2, hd), BF16),
                pltpu.VMEM((rows * TILE, hd), F32),
                pltpu.VMEM((nt, rows, TILE, hd), BF16),
                dma((nt, 3)), dma((nt, nx)), dma((nt, nx)), dma((nt, nx, 2)), dma((nslot, ny, nx)), dma((ny, nx)),
                dma((nslot, ny, nx)), dma((nslot, ny, nx)), dma((nslot, ny, nx)), dma((nt, TILE)), dma((nt,)),
            ],
            compiler_params=pltpu.CompilerParams(collective_id=0, has_side_effects=True, vmem_limit_bytes=56 * 1024 * 1024),
        )(q, k, v)

    return jax.shard_map(local, mesh=mesh, in_specs=(spec, spec, spec), out_specs=spec, check_vma=False)
```

```python
import functools
import math

import jax
import jax.numpy as jnp
from jax import lax
from jax.experimental import pallas as pl
from jax.experimental.pallas import tpu as pltpu
from jax.sharding import PartitionSpec as P

MESH = pl.DeviceIdType.MESH
NEG = -1.0e30
TILE = 8
F32 = jnp.float32
BF16 = jnp.bfloat16


def kernel(ny, nx, nt, scale, q_hbm, k_hbm, v_hbm, o_hbm, tin, xs, send, r1, qkv, sbuf, bias, ostage, orecv, ys, tout,
           in_sem, s1, q1, s2, q2, sx, fsend, frecv, osend, orecv_sem, out_sem):
    rows = q_hbm.shape[0]
    c2 = rows // 2
    hd = q_hbm.shape[2]
    cy = lax.axis_index("cy")
    cx = lax.axis_index("cx")
    x = cx // 2
    c = lax.rem(cx, 2)
    odd = lax.rem(x + cy, 2)
    mate = cy + 1 - 2 * lax.rem(cy, 2)
    across = ny - 1 - cy
    inner = lax.rem((cy + 1) // 2, 2)

    def dev(xd, yd, core):
        return {"cy": yd, "cx": xd * 2 + core}

    nslot = (nt - 1) // 2

    def slot_of(t):
        return jnp.where(t == 0, nslot, (t - 1) // 2)

    def owner_row(t, xd, h, y, inn):
        shared = jnp.where(inn == h, y, y + 1 - 2 * lax.rem(y, 2))
        return jnp.where(t == 0, shared, lax.rem(xd + t, 2) + 2 * h)

    def in_copy(t, j):
        src = (q_hbm, k_hbm, v_hbm)[j]
        return pltpu.make_async_copy(src.at[:, pl.ds(pl.multiple_of(t * TILE, TILE), TILE), :], tin.at[t, j], in_sem.at[t, j])

    bar = pltpu.get_barrier_semaphore()
    for i in range(1, nx):
        pl.semaphore_signal(bar, inc=1, device_id=dev(lax.rem(x + i, nx), cy, c), device_id_type=MESH)
    for i in range(1, ny):
        pl.semaphore_signal(bar, inc=1, device_id=dev(x, lax.rem(cy + i, ny), c), device_id_type=MESH)
    pl.semaphore_signal(bar, inc=1, device_id=dev(x, cy, 1 - c), device_id_type=MESH)

    for t in range(nt):
        for j in range(3):
            in_copy(t, j).start()

    def x_copy(t, xd):
        return pltpu.make_async_remote_copy(
            src_ref=send.at[t, xd], dst_ref=r1.at[t, x], send_sem=s1.at[t, xd], recv_sem=q1.at[t, x],
            device_id=dev(xd, cy, c), device_id_type=MESH)

    def gray(i):
        return jnp.where(i < 2, i, 5 - i)

    def load_tile(t, u):
        for j in range(3):
            in_copy(t, j).wait()
            xs[u, j] = tin[t, j].astype(F32).reshape(rows * TILE, hd)

    def head_rows(u, j, k):
        return xs[u, j, pl.ds(k, rows, stride=TILE), :].astype(BF16).reshape(2, c2, hd)

    def send_tiles(t, n):
        def one(i, _):
            xd = lax.rem(x + gray(i), nx)
            for u in range(n):
                for h in range(2):
                    for j in range(3):
                        send[t + u, xd, h, j] = head_rows(u, j, 2 * xd + h)
                x_copy(t + u, xd).start()
            return 0

        lax.fori_loop(1, nx, one, 0)
        for u in range(n):
            for h in range(2):
                for j in range(3):
                    r1[t + u, x, h, j] = head_rows(u, j, 2 * x + h)

    load_tile(0, 0)

    qi = lax.broadcasted_iota(jnp.int32, (nx * c2, 2 * nx * c2), 0)
    ki = lax.broadcasted_iota(jnp.int32, (nx * c2, 2 * nx * c2), 1)
    qsp = 2 * (qi // c2) + c
    ksp = 2 * ((ki // c2) % nx) + ki // (nx * c2)
    qr = qi % c2
    kr = ki % c2
    low = (ksp < qsp) | ((ksp == qsp) & (kr <= qr))
    high = (ksp > qsp) | ((ksp == qsp) & (kr <= qr))
    bias[0] = jnp.where(low, 0.0, NEG)
    bias[1] = jnp.where(high, 0.0, NEG)

    pl.semaphore_wait(bar, nx + ny - 1)
    send_tiles(0, 1)

    def send_rest(i, _):
        load_tile(2 * i + 1, 0)
        load_tile(2 * i + 2, 1)
        send_tiles(2 * i + 1, 2)
        return 0

    lax.fori_loop(0, nslot, send_rest, 0)

    def y_copy(t, sx_, h, yd):
        slot = slot_of(t)
        return pltpu.make_async_remote_copy(
            src_ref=r1.at[t, sx_, h], dst_ref=qkv.at[slot, c, cy, sx_], send_sem=s2.at[t, sx_, h],
            recv_sem=q2.at[slot, cy, sx_], device_id=dev(x, yd, c), device_id_type=MESH)

    def y_recv(slot, sy, sx_):
        return pltpu.make_async_remote_copy(
            src_ref=qkv.at[slot, c, sy, sx_], dst_ref=qkv.at[slot, c, sy, sx_], send_sem=s2.at[0, 0, 0],
            recv_sem=q2.at[slot, sy, sx_], device_id=dev(x, cy, 1 - c), device_id_type=MESH)

    def kv_view(ref, full):
        return ref.at[pl.ds(1, 2)] if full else ref.at[pl.ds(1, 2), 0]

    def cross_copy(src, sy, sx_, full):
        return pltpu.make_async_remote_copy(
            src_ref=kv_view(src, full), dst_ref=kv_view(qkv.at[nslot, c, sy, sx_], full), send_sem=sx.at[sy, sx_],
            recv_sem=q2.at[nslot, sy, sx_], device_id=dev(x, across, c), device_id_type=MESH)

    def core_copy(src, slot, sy, sx_, core, full):
        return pltpu.make_async_remote_copy(
            src_ref=kv_view(src, full), dst_ref=kv_view(qkv.at[slot, core, sy, sx_], full), send_sem=fsend.at[slot, sy, sx_],
            recv_sem=frecv.at[slot, sy, sx_], device_id=dev(x, cy, 1 - c), device_id_type=MESH)

    def either(full, act):
        @pl.when(full)
        def _():
            act(True)

        @pl.when(jnp.logical_not(full))
        def _():
            act(False)

    outer = cy < ny // 2

    def cross(src, sy, sx_):
        either(jnp.logical_not(outer), lambda full: cross_copy(src, sy, sx_, full).start())

    def relay(t, i):
        sx_ = lax.rem(x + gray(i), nx)

        @pl.when(sx_ != x)
        def _():
            pltpu.make_async_remote_copy(
                src_ref=send.at[t, 0], dst_ref=r1.at[t, sx_], send_sem=s1.at[0, 0], recv_sem=q1.at[t, sx_],
                device_id=dev(x, cy, 1 - c), device_id_type=MESH).wait_recv()

        slot = slot_of(t)
        for h in range(2):
            yd = owner_row(t, x, h, cy, inner)

            @pl.when(yd != cy)
            def _():
                y_copy(t, sx_, h, yd).start()

            @pl.when(yd == cy)
            def _():
                core_copy(r1.at[t, sx_, h], slot, cy, sx_, c, True).start()

                @pl.when(t == 0)
                def _():
                    cross(r1.at[t, sx_, h], cy, sx_)

                qkv[slot, c, cy, sx_] = r1[t, sx_, h]

    def share_first(i):
        sx_ = lax.rem(x + gray(i), nx)
        y_recv(nslot, mate, sx_).wait_recv()
        core_copy(qkv.at[nslot, c, mate, sx_], nslot, mate, sx_, c, True).start()
        cross(qkv.at[nslot, c, mate, sx_], mate, sx_)

    def share_second(i):
        sx_ = lax.rem(x + gray(i), nx)
        for sy in (across, across + 1 - 2 * lax.rem(across, 2)):
            def act(full):
                cross_copy(qkv.at[nslot, c, sy, sx_], sy, sx_, full).wait_recv()
                core_copy(qkv.at[nslot, c, sy, sx_], nslot, sy, sx_, c, full).start()

            either(outer, act)
        return 0

    def full_rows(slot, sy):
        return (slot < nslot) | outer | (sy >= ny // 2)

    def arrived(slot):
        def one(i, _):
            sy = i // nx
            sx_ = lax.rem(i, nx)
            either(full_rows(slot, sy), lambda full: core_copy(qkv.at[slot, 1 - c, sy, sx_], slot, sy, sx_, 1 - c, full).wait_recv())
            return 0

        lax.fori_loop(0, nx * ny, one, 0)

    def gather(slot):
        def one(i, _):
            sy = lax.rem(cy + i // nx, ny)
            sx_ = lax.rem(x + gray(lax.rem(i, nx)), nx)
            y_recv(slot, sy, sx_).wait_recv()
            core_copy(qkv.at[slot, c, sy, sx_], slot, sy, sx_, c, True).start()
            return 0

        lax.fori_loop(nx, nx * ny, one, 0)

    def tile_of(slot):
        return jnp.where(slot == nslot, 0, 2 * slot + 2 - odd)

    def my_head(slot):
        return 2 * x + jnp.where(slot == nslot, inner, cy // 2)

    def o_copy(slot, sy, sx_):
        t = tile_of(slot)
        k = my_head(slot)
        return pltpu.make_async_remote_copy(
            src_ref=ostage.at[slot, sy, sx_], dst_ref=orecv.at[t, k], send_sem=osend.at[slot, sy, sx_],
            recv_sem=orecv_sem.at[t, k], device_id=dev(sx_, sy, c), device_id_type=MESH)

    def band(slot, b, j):
        half = b // ny
        yk = b if half == 0 else 2 * ny - 1 - b
        return qkv[slot, :, yk, :, j, half].reshape(2 * nx * c2, hd)

    def scores(q, k):
        return lax.dot_general(q, k, (((1,), (1,)), ((), ())), preferred_element_type=F32) * scale

    def lanes(s, op):
        r = s[:, :hd]
        for i in range(1, s.shape[1] // hd):
            r = op(r, s[:, i * hd:(i + 1) * hd])
        return r

    def attend(slot, pair):
        for p in range(ny // 2):
            @pl.when(pair == p)
            def _():
                attend_rows(slot, (2 * p, 2 * p + 1))

    def attend_rows(slot, source_rows):
        tiles = [(y, half, 2 * ny - y if half else y + 1) for half in (1, 0) for y in source_rows]
        tiles.sort(key=lambda t: -t[2])
        start = [sum(t[2] for t in tiles[:i]) for i in range(len(tiles) + 1)]
        top = [None] * len(tiles)
        total = [None] * len(tiles)

        def score(i, b):
            y, half, nb = tiles[i]
            q = qkv[slot, c, y, :, 0, half].reshape(nx * c2, hd)
            s = scores(q, band(slot, b, 1))
            if b == nb - 1:
                s = s + bias[half]
            sbuf[start[i] + b] = s
            t = lanes(s, jnp.maximum)
            top[i] = t if top[i] is None else jnp.maximum(top[i], t)

        def weigh(i, b, m):
            p = jnp.exp2(sbuf[start[i] + b] - m)
            l = lanes(p, jnp.add)
            pv = jnp.dot(p.astype(BF16), band(slot, b, 2), preferred_element_type=F32)
            total[i] = (l, pv) if total[i] is None else (total[i][0] + l, total[i][1] + pv)

        for b in range(tiles[0][2]):
            score(0, b)
        for i, (y, half, nb) in enumerate(tiles):
            m = jnp.broadcast_to(jnp.max(top[i], axis=-1, keepdims=True), (nx * c2, hd))
            m = jnp.concatenate([m] * (sbuf.shape[2] // hd), axis=1)
            nxt = tiles[i + 1][2] if i + 1 < len(tiles) else 0
            for b in range(max(nb, nxt)):
                if b < nxt:
                    score(i + 1, b)
                if b < nb:
                    weigh(i, b, m)
            l, acc = total[i]
            o = acc / jnp.sum(l, axis=-1, keepdims=True)
            ostage[slot, y, :, half] = o.astype(BF16).reshape(nx, c2, hd)

    def send_back(slot, y):
        def back(sx_, _):
            mine = (sx_ == x) & (y == cy)

            @pl.when(jnp.logical_not(mine))
            def _():
                o_copy(slot, y, sx_).start()

            @pl.when(mine)
            def _():
                orecv[tile_of(slot), my_head(slot)] = ostage[slot, y, sx_]
            return 0

        lax.fori_loop(0, nx, back, 0)
        return 0

    def relay_two(n, i):
        relay(2 * n + 1, i)
        relay(2 * n + 2, i)

    relay(0, 0)
    relay_two(0, 0)

    def first(i, _):
        @pl.when(i < nx)
        def _():
            relay(0, i)

        @pl.when(i == nx - 1)
        def _():
            relay_two(1, 0)

        share_first(i - 1)
        return 0

    lax.fori_loop(1, nx + 1, first, 0)
    lax.fori_loop(1, nx, lambda i, _: (relay_two(0, i), 0)[1], 0)
    lax.fori_loop(0, nx, lambda i, _: share_second(i), 0)

    def step(n, _):
        pairs = ny // 2
        slot = jnp.where(n == 0, nslot, (n - 1) // pairs)
        pair = jnp.where(n == 0, cy // 2, lax.rem(n + 1, pairs))

        @pl.when(n == 0)
        def _():
            relay_two(1, 1)

        @pl.when(n == 1)
        def _():
            relay_two(1, 2)
            relay_two(1, 3)

        @pl.when((n == 1) | (n == 1 + pairs))
        def _():
            gather(slot)

        @pl.when(n != 2)
        def _():
            @pl.when(n != 2 + pairs)
            def _():
                arrived(slot)

        attend(slot, pair)
        send_back(slot, 2 * pair)
        send_back(slot, 2 * pair + 1)
        return 0

    lax.fori_loop(0, 1 + nslot * ny // 2, step, 0)

    def out_copy(t):
        return pltpu.make_async_copy(tout.at[t], o_hbm.at[:, pl.ds(pl.multiple_of(t * TILE, TILE), TILE), :], out_sem.at[t])

    def out_tile(t, _):
        def one(k, _):
            xd = k // 2
            yd = owner_row(t, xd, lax.rem(k, 2), cy, inner)

            @pl.when((xd != x) | (yd != cy))
            def _():
                pltpu.make_async_remote_copy(
                    src_ref=orecv.at[t, k], dst_ref=orecv.at[t, k], send_sem=osend.at[0, 0, 0],
                    recv_sem=orecv_sem.at[t, k], device_id=dev(x, cy, 1 - c), device_id_type=MESH).wait_recv()

            ys[pl.ds(k, rows, stride=TILE), :] = orecv[t, k].reshape(rows, hd).astype(F32)
            return 0

        lax.fori_loop(0, TILE, one, 0)
        tout[t] = ys[...].reshape(rows, TILE, hd).astype(BF16)
        out_copy(t).start()
        return 0

    lax.fori_loop(0, nt, out_tile, 0)

    def sent(t, _):
        def one(i, _):
            xd = lax.rem(x + i, nx)

            @pl.when(i > 0)
            def _():
                x_copy(t, xd).wait_send()

            for h in range(2):
                yd = owner_row(t, x, h, cy, inner)

                @pl.when(yd != cy)
                def _():
                    y_copy(t, xd, h, yd).wait_send()
            return 0

        lax.fori_loop(0, nx, one, 0)
        out_copy(t).wait()
        return 0

    lax.fori_loop(0, nt, sent, 0)

    def drained(slot, _):
        def one(i, _):
            sy = i // nx
            sx_ = lax.rem(i, nx)
            mine = (sy // 2) == (cy // 2)
            either(full_rows(slot, sy), lambda full: core_copy(qkv.at[slot, c, sy, sx_], slot, sy, sx_, c, full).wait_send())

            @pl.when((slot == nslot) & mine)
            def _():
                either(jnp.logical_not(outer), lambda full: cross_copy(qkv.at[nslot, c, sy, sx_], sy, sx_, full).wait_send())

            @pl.when(((slot < nslot) | mine) & ((sy != cy) | (sx_ != x)))
            def _():
                o_copy(slot, sy, sx_).wait_send()
            return 0

        lax.fori_loop(0, nx * ny, one, 0)
        return 0

    lax.fori_loop(0, nslot + 1, drained, 0)


def solution(mesh):
    ny = mesh.shape['cy']
    nx = mesh.shape['cx'] // 2
    spec = P(('dp', 'cy', 'cx'))

    def local(q, k, v):
        rows, nh, hd = q.shape
        c2 = rows // 2
        nt = nh // TILE
        nslot = (nt + 1) // 2
        scale = hd ** -0.5 * math.log2(math.e)
        dma = pltpu.SemaphoreType.DMA
        return pl.pallas_call(
            functools.partial(kernel, ny, nx, nt, scale),
            out_shape=jax.ShapeDtypeStruct(q.shape, q.dtype),
            in_specs=[pl.BlockSpec(memory_space=pl.ANY)] * 3,
            out_specs=pl.BlockSpec(memory_space=pl.ANY),
            scratch_shapes=[
                pltpu.VMEM((nt, 3, rows, TILE, hd), BF16),
                pltpu.VMEM((2, 3, rows * TILE, hd), F32),
                pltpu.VMEM((nt, nx, 2, 3, 2, c2, hd), BF16),
                pltpu.VMEM((nt, nx, 2, 3, 2, c2, hd), BF16),
                pltpu.VMEM((nslot, 2, ny, nx, 3, 2, c2, hd), BF16),
                pltpu.VMEM((4 * ny + 2, nx * c2, 2 * nx * c2), F32),
                pltpu.VMEM((2, nx * c2, 2 * nx * c2), F32),
                pltpu.VMEM((nslot, ny, nx, 2, c2, hd), BF16),
                pltpu.VMEM((nt, TILE, 2, c2, hd), BF16),
                pltpu.VMEM((rows * TILE, hd), F32),
                pltpu.VMEM((nt, rows, TILE, hd), BF16),
                dma((nt, 3)), dma((nt, nx)), dma((nt, nx)), dma((nt, nx, 2)), dma((nslot, ny, nx)), dma((ny, nx)),
                dma((nslot, ny, nx)), dma((nslot, ny, nx)), dma((nslot, ny, nx)), dma((nt, TILE)), dma((nt,)),
            ],
            compiler_params=pltpu.CompilerParams(collective_id=0, has_side_effects=True, vmem_limit_bytes=56 * 1024 * 1024),
        )(q, k, v)

    return jax.shard_map(local, mesh=mesh, in_specs=(spec, spec, spec), out_specs=spec, check_vma=False)
```

```python
import functools
import math

import jax
import jax.numpy as jnp
from jax import lax
from jax.experimental import pallas as pl
from jax.experimental.pallas import tpu as pltpu
from jax.sharding import PartitionSpec as P

MESH = pl.DeviceIdType.MESH
NEG = -1.0e30
TILE = 8
F32 = jnp.float32
BF16 = jnp.bfloat16


def kernel(ny, nx, nt, scale, q_hbm, k_hbm, v_hbm, o_hbm, tin, xs, send, r1, qkv, sbuf, bias, ostage, orecv, ys, tout,
           in_sem, s1, q1, s2, q2, sx, fsend, frecv, osend, orecv_sem, out_sem):
    rows = q_hbm.shape[0]
    c2 = rows // 2
    hd = q_hbm.shape[2]
    cy = lax.axis_index("cy")
    cx = lax.axis_index("cx")
    x = cx // 2
    c = lax.rem(cx, 2)
    odd = lax.rem(x + cy, 2)
    mate = cy + 1 - 2 * lax.rem(cy, 2)
    across = ny - 1 - cy
    inner = lax.rem((cy + 1) // 2, 2)

    def dev(xd, yd, core):
        return {"cy": yd, "cx": xd * 2 + core}

    nslot = (nt - 1) // 2

    def slot_of(t):
        return jnp.where(t == 0, nslot, (t - 1) // 2)

    def owner_row(t, xd, h, y, inn):
        shared = jnp.where(inn == h, y, y + 1 - 2 * lax.rem(y, 2))
        return jnp.where(t == 0, shared, lax.rem(xd + t, 2) + 2 * h)

    def in_copy(t, j):
        src = (q_hbm, k_hbm, v_hbm)[j]
        return pltpu.make_async_copy(src.at[:, pl.ds(pl.multiple_of(t * TILE, TILE), TILE), :], tin.at[t, j], in_sem.at[t, j])

    bar = pltpu.get_barrier_semaphore()
    for i in range(1, nx):
        pl.semaphore_signal(bar, inc=1, device_id=dev(lax.rem(x + i, nx), cy, c), device_id_type=MESH)
    for i in range(1, ny):
        pl.semaphore_signal(bar, inc=1, device_id=dev(x, lax.rem(cy + i, ny), c), device_id_type=MESH)
    pl.semaphore_signal(bar, inc=1, device_id=dev(x, cy, 1 - c), device_id_type=MESH)

    for t in range(nt):
        for j in range(3):
            in_copy(t, j).start()

    def x_copy(t, xd):
        return pltpu.make_async_remote_copy(
            src_ref=send.at[t, xd], dst_ref=r1.at[t, x], send_sem=s1.at[t, xd], recv_sem=q1.at[t, x],
            device_id=dev(xd, cy, c), device_id_type=MESH)

    def gray(i):
        return jnp.where(i < 2, i, 5 - i)

    def load_tile(t, u):
        for j in range(3):
            in_copy(t, j).wait()
            xs[u, j] = tin[t, j].astype(F32).reshape(rows * TILE, hd)

    def head_rows(u, j, k):
        return xs[u, j, pl.ds(k, rows, stride=TILE), :].astype(BF16).reshape(2, c2, hd)

    def send_tiles(t, n):
        def one(i, _):
            xd = lax.rem(x + gray(i), nx)
            for u in range(n):
                for h in range(2):
                    for j in range(3):
                        send[t + u, xd, h, j] = head_rows(u, j, 2 * xd + h)
                x_copy(t + u, xd).start()
            return 0

        lax.fori_loop(1, nx, one, 0)
        for u in range(n):
            for h in range(2):
                for j in range(3):
                    r1[t + u, x, h, j] = head_rows(u, j, 2 * x + h)

    load_tile(0, 0)

    qi = lax.broadcasted_iota(jnp.int32, (nx * c2, 2 * nx * c2), 0)
    ki = lax.broadcasted_iota(jnp.int32, (nx * c2, 2 * nx * c2), 1)
    qsp = 2 * (qi // c2) + c
    ksp = 2 * ((ki // c2) % nx) + ki // (nx * c2)
    qr = qi % c2
    kr = ki % c2
    low = (ksp < qsp) | ((ksp == qsp) & (kr <= qr))
    high = (ksp > qsp) | ((ksp == qsp) & (kr <= qr))
    bias[0] = jnp.where(low, 0.0, NEG)
    bias[1] = jnp.where(high, 0.0, NEG)

    pl.semaphore_wait(bar, nx + ny - 1)
    send_tiles(0, 1)

    def send_rest(i, _):
        load_tile(2 * i + 1, 0)
        load_tile(2 * i + 2, 1)
        send_tiles(2 * i + 1, 2)
        return 0

    lax.fori_loop(0, nslot, send_rest, 0)

    def y_copy(t, sx_, h, yd):
        slot = slot_of(t)
        return pltpu.make_async_remote_copy(
            src_ref=r1.at[t, sx_, h], dst_ref=qkv.at[slot, c, cy, sx_], send_sem=s2.at[t, sx_, h],
            recv_sem=q2.at[slot, cy, sx_], device_id=dev(x, yd, c), device_id_type=MESH)

    def y_recv(slot, sy, sx_):
        return pltpu.make_async_remote_copy(
            src_ref=qkv.at[slot, c, sy, sx_], dst_ref=qkv.at[slot, c, sy, sx_], send_sem=s2.at[0, 0, 0],
            recv_sem=q2.at[slot, sy, sx_], device_id=dev(x, cy, 1 - c), device_id_type=MESH)

    def kv_view(ref, full):
        return ref.at[pl.ds(1, 2)] if full else ref.at[pl.ds(1, 2), 0]

    def cross_copy(src, sy, sx_, full):
        return pltpu.make_async_remote_copy(
            src_ref=kv_view(src, full), dst_ref=kv_view(qkv.at[nslot, c, sy, sx_], full), send_sem=sx.at[sy, sx_],
            recv_sem=q2.at[nslot, sy, sx_], device_id=dev(x, across, c), device_id_type=MESH)

    def core_copy(src, slot, sy, sx_, core, full):
        return pltpu.make_async_remote_copy(
            src_ref=kv_view(src, full), dst_ref=kv_view(qkv.at[slot, core, sy, sx_], full), send_sem=fsend.at[slot, sy, sx_],
            recv_sem=frecv.at[slot, sy, sx_], device_id=dev(x, cy, 1 - c), device_id_type=MESH)

    def either(full, act):
        @pl.when(full)
        def _():
            act(True)

        @pl.when(jnp.logical_not(full))
        def _():
            act(False)

    outer = cy < ny // 2

    def cross(src, sy, sx_):
        either(jnp.logical_not(outer), lambda full: cross_copy(src, sy, sx_, full).start())

    def relay(t, i):
        sx_ = lax.rem(x + gray(i), nx)

        @pl.when(sx_ != x)
        def _():
            pltpu.make_async_remote_copy(
                src_ref=send.at[t, 0], dst_ref=r1.at[t, sx_], send_sem=s1.at[0, 0], recv_sem=q1.at[t, sx_],
                device_id=dev(x, cy, 1 - c), device_id_type=MESH).wait_recv()

        slot = slot_of(t)
        for h in range(2):
            yd = owner_row(t, x, h, cy, inner)

            @pl.when(yd != cy)
            def _():
                y_copy(t, sx_, h, yd).start()

            @pl.when(yd == cy)
            def _():
                core_copy(r1.at[t, sx_, h], slot, cy, sx_, c, True).start()

                @pl.when(t == 0)
                def _():
                    cross(r1.at[t, sx_, h], cy, sx_)

                qkv[slot, c, cy, sx_] = r1[t, sx_, h]

    def share_first(i):
        sx_ = lax.rem(x + gray(i), nx)
        y_recv(nslot, mate, sx_).wait_recv()
        core_copy(qkv.at[nslot, c, mate, sx_], nslot, mate, sx_, c, True).start()
        cross(qkv.at[nslot, c, mate, sx_], mate, sx_)

    def share_second(i):
        sx_ = lax.rem(x + gray(i), nx)
        for sy in (across, across + 1 - 2 * lax.rem(across, 2)):
            def act(full):
                cross_copy(qkv.at[nslot, c, sy, sx_], sy, sx_, full).wait_recv()
                core_copy(qkv.at[nslot, c, sy, sx_], nslot, sy, sx_, c, full).start()

            either(outer, act)
        return 0

    def full_rows(slot, sy):
        return (slot < nslot) | outer | (sy >= ny // 2)

    def arrived(slot):
        def one(i, _):
            sy = i // nx
            sx_ = lax.rem(i, nx)
            either(full_rows(slot, sy), lambda full: core_copy(qkv.at[slot, 1 - c, sy, sx_], slot, sy, sx_, 1 - c, full).wait_recv())
            return 0

        lax.fori_loop(0, nx * ny, one, 0)

    def gather(slot):
        def one(i, _):
            sy = lax.rem(cy + i // nx, ny)
            sx_ = lax.rem(x + gray(lax.rem(i, nx)), nx)
            y_recv(slot, sy, sx_).wait_recv()
            core_copy(qkv.at[slot, c, sy, sx_], slot, sy, sx_, c, True).start()
            return 0

        lax.fori_loop(nx, nx * ny, one, 0)

    def tile_of(slot):
        return jnp.where(slot == nslot, 0, 2 * slot + 2 - odd)

    def my_head(slot):
        return 2 * x + jnp.where(slot == nslot, inner, cy // 2)

    def o_copy(slot, sy, sx_):
        t = tile_of(slot)
        k = my_head(slot)
        return pltpu.make_async_remote_copy(
            src_ref=ostage.at[slot, sy, sx_], dst_ref=orecv.at[t, k], send_sem=osend.at[slot, sy, sx_],
            recv_sem=orecv_sem.at[t, k], device_id=dev(sx_, sy, c), device_id_type=MESH)

    def band(slot, b, j):
        half = b // ny
        yk = b if half == 0 else 2 * ny - 1 - b
        return qkv[slot, :, yk, :, j, half].reshape(2 * nx * c2, hd)

    def scores(q, k):
        return lax.dot_general(q, k, (((1,), (1,)), ((), ())), preferred_element_type=F32) * scale

    def lanes(s, op):
        r = s[:, :hd]
        for i in range(1, s.shape[1] // hd):
            r = op(r, s[:, i * hd:(i + 1) * hd])
        return r

    def attend(slot, pair):
        for p in range(ny // 2):
            @pl.when(pair == p)
            def _():
                attend_rows(slot, (2 * p, 2 * p + 1))

    def attend_rows(slot, source_rows):
        tiles = [(y, half, 2 * ny - y if half else y + 1) for half in (1, 0) for y in source_rows]
        tiles.sort(key=lambda t: -t[2])
        start = [sum(t[2] for t in tiles[:i]) for i in range(len(tiles) + 1)]
        top = [None] * len(tiles)
        total = [None] * len(tiles)

        def score(i, b):
            y, half, nb = tiles[i]
            q = qkv[slot, c, y, :, 0, half].reshape(nx * c2, hd)
            s = scores(q, band(slot, b, 1))
            if b == nb - 1:
                s = s + bias[half]
            sbuf[start[i] + b] = s
            t = lanes(s, jnp.maximum)
            top[i] = t if top[i] is None else jnp.maximum(top[i], t)

        def weigh(i, b, m):
            p = jnp.exp2(sbuf[start[i] + b] - m)
            l = lanes(p, jnp.add)
            pv = jnp.dot(p.astype(BF16), band(slot, b, 2), preferred_element_type=F32)
            total[i] = (l, pv) if total[i] is None else (total[i][0] + l, total[i][1] + pv)

        for b in range(tiles[0][2]):
            score(0, b)
        for i, (y, half, nb) in enumerate(tiles):
            m = jnp.broadcast_to(jnp.max(top[i], axis=-1, keepdims=True), (nx * c2, hd))
            m = jnp.concatenate([m] * (sbuf.shape[2] // hd), axis=1)
            nxt = tiles[i + 1][2] if i + 1 < len(tiles) else 0
            for b in range(max(nb, nxt)):
                if b < nxt:
                    score(i + 1, b)
                if b < nb:
                    weigh(i, b, m)
            l, acc = total[i]
            o = acc / jnp.sum(l, axis=-1, keepdims=True)
            ostage[slot, y, :, half] = o.astype(BF16).reshape(nx, c2, hd)
            if y not in [t[0] for t in tiles[i + 1:]]:
                send_back(slot, y)

    def send_back(slot, y):
        def back(sx_, _):
            mine = (sx_ == x) & (y == cy)

            @pl.when(jnp.logical_not(mine))
            def _():
                o_copy(slot, y, sx_).start()

            @pl.when(mine)
            def _():
                orecv[tile_of(slot), my_head(slot)] = ostage[slot, y, sx_]
            return 0

        lax.fori_loop(0, nx, back, 0)
        return 0

    def relay_two(n, i):
        relay(2 * n + 1, i)
        relay(2 * n + 2, i)

    relay(0, 0)
    relay_two(0, 0)

    def first(i, _):
        @pl.when(i < nx)
        def _():
            relay(0, i)

        @pl.when(i == nx - 1)
        def _():
            relay_two(1, 0)

        share_first(i - 1)
        return 0

    lax.fori_loop(1, nx + 1, first, 0)
    lax.fori_loop(1, nx, lambda i, _: (relay_two(0, i), 0)[1], 0)
    lax.fori_loop(0, nx, lambda i, _: share_second(i), 0)

    def step(n, _):
        pairs = ny // 2
        slot = jnp.where(n == 0, nslot, (n - 1) // pairs)
        pair = jnp.where(n == 0, cy // 2, lax.rem(n + 1, pairs))

        @pl.when(n == 0)
        def _():
            relay_two(1, 1)

        @pl.when(n == 1)
        def _():
            relay_two(1, 2)
            relay_two(1, 3)

        @pl.when((n == 1) | (n == 1 + pairs))
        def _():
            gather(slot)

        @pl.when(n != 2)
        def _():
            @pl.when(n != 2 + pairs)
            def _():
                arrived(slot)

        attend(slot, pair)
        return 0

    lax.fori_loop(0, 1 + nslot * ny // 2, step, 0)

    def out_copy(t):
        return pltpu.make_async_copy(tout.at[t], o_hbm.at[:, pl.ds(pl.multiple_of(t * TILE, TILE), TILE), :], out_sem.at[t])

    def out_tile(t, _):
        def one(k, _):
            xd = k // 2
            yd = owner_row(t, xd, lax.rem(k, 2), cy, inner)

            @pl.when((xd != x) | (yd != cy))
            def _():
                pltpu.make_async_remote_copy(
                    src_ref=orecv.at[t, k], dst_ref=orecv.at[t, k], send_sem=osend.at[0, 0, 0],
                    recv_sem=orecv_sem.at[t, k], device_id=dev(x, cy, 1 - c), device_id_type=MESH).wait_recv()

            ys[pl.ds(k, rows, stride=TILE), :] = orecv[t, k].reshape(rows, hd).astype(F32)
            return 0

        lax.fori_loop(0, TILE, one, 0)
        tout[t] = ys[...].reshape(rows, TILE, hd).astype(BF16)
        out_copy(t).start()
        return 0

    lax.fori_loop(0, nt, out_tile, 0)

    def sent(t, _):
        def one(i, _):
            xd = lax.rem(x + i, nx)

            @pl.when(i > 0)
            def _():
                x_copy(t, xd).wait_send()

            for h in range(2):
                yd = owner_row(t, x, h, cy, inner)

                @pl.when(yd != cy)
                def _():
                    y_copy(t, xd, h, yd).wait_send()
            return 0

        lax.fori_loop(0, nx, one, 0)
        out_copy(t).wait()
        return 0

    lax.fori_loop(0, nt, sent, 0)

    def drained(slot, _):
        def one(i, _):
            sy = i // nx
            sx_ = lax.rem(i, nx)
            mine = (sy // 2) == (cy // 2)
            either(full_rows(slot, sy), lambda full: core_copy(qkv.at[slot, c, sy, sx_], slot, sy, sx_, c, full).wait_send())

            @pl.when((slot == nslot) & mine)
            def _():
                either(jnp.logical_not(outer), lambda full: cross_copy(qkv.at[nslot, c, sy, sx_], sy, sx_, full).wait_send())

            @pl.when(((slot < nslot) | mine) & ((sy != cy) | (sx_ != x)))
            def _():
                o_copy(slot, sy, sx_).wait_send()
            return 0

        lax.fori_loop(0, nx * ny, one, 0)
        return 0

    lax.fori_loop(0, nslot + 1, drained, 0)


def solution(mesh):
    ny = mesh.shape['cy']
    nx = mesh.shape['cx'] // 2
    spec = P(('dp', 'cy', 'cx'))

    def local(q, k, v):
        rows, nh, hd = q.shape
        c2 = rows // 2
        nt = nh // TILE
        nslot = (nt + 1) // 2
        scale = hd ** -0.5 * math.log2(math.e)
        dma = pltpu.SemaphoreType.DMA
        return pl.pallas_call(
            functools.partial(kernel, ny, nx, nt, scale),
            out_shape=jax.ShapeDtypeStruct(q.shape, q.dtype),
            in_specs=[pl.BlockSpec(memory_space=pl.ANY)] * 3,
            out_specs=pl.BlockSpec(memory_space=pl.ANY),
            scratch_shapes=[
                pltpu.VMEM((nt, 3, rows, TILE, hd), BF16),
                pltpu.VMEM((2, 3, rows * TILE, hd), F32),
                pltpu.VMEM((nt, nx, 2, 3, 2, c2, hd), BF16),
                pltpu.VMEM((nt, nx, 2, 3, 2, c2, hd), BF16),
                pltpu.VMEM((nslot, 2, ny, nx, 3, 2, c2, hd), BF16),
                pltpu.VMEM((4 * ny + 2, nx * c2, 2 * nx * c2), F32),
                pltpu.VMEM((2, nx * c2, 2 * nx * c2), F32),
                pltpu.VMEM((nslot, ny, nx, 2, c2, hd), BF16),
                pltpu.VMEM((nt, TILE, 2, c2, hd), BF16),
                pltpu.VMEM((rows * TILE, hd), F32),
                pltpu.VMEM((nt, rows, TILE, hd), BF16),
                dma((nt, 3)), dma((nt, nx)), dma((nt, nx)), dma((nt, nx, 2)), dma((nslot, ny, nx)), dma((ny, nx)),
                dma((nslot, ny, nx)), dma((nslot, ny, nx)), dma((nslot, ny, nx)), dma((nt, TILE)), dma((nt,)),
            ],
            compiler_params=pltpu.CompilerParams(collective_id=0, has_side_effects=True, vmem_limit_bytes=56 * 1024 * 1024),
        )(q, k, v)

    return jax.shard_map(local, mesh=mesh, in_specs=(spec, spec, spec), out_specs=spec, check_vma=False)
```
